256 devices in a mesh: row: 32 (over y, x, core), col: 8 (over z).
Axes of the slice: x: 4, y: 4, z: 8, core: 2. Of those that a mesh axis runs over, the one named last changes fastest.
Arguments:
- features: bfloat16 [262144, 256], P(('col', 'row')), may hold values from -6 to 6
- block_values: bfloat16 [32, 8, 192, 128, 128], P('row', 'col'), may hold values from -0.1875 to 0.1875
- row_ptr: int32 [32, 8, 65], P('row', 'col'), may hold values from 0 to 144, as said below
- block_cols: int32 [32, 8, 192], P('row', 'col'), may hold values from 0 to 2047, as said below
Outputs:
- product: bfloat16 [262144, 256], P(('row', 'col'))
The draws below stay inside these ranges and needn't reach their ends.
Inputs may be any that keep to these rules, and one draw needn't show every extreme that they name: row_ptr[r, c, 0] = 0, row_ptr never falls along its last dimension, row_ptr[r, c, 64] <= 144, and on exactly one device row_ptr[r, c, 64] = 144. block_cols[r, c, s] lies in c * 256 to (c + 1) * 256 - 1; a block column may repeat within a block row, and repeated blocks add.
All inputs are finite; a program needn't handle non-finite values.
Results may differ from the reference program's by a relative error of at most 0.001.
Values may be sent and summed in bfloat16 or wider, within the bound.
A program may use at most 128 MiB of HBM per device.

```python
import jax
import jax.numpy as jnp
from jax import lax

B = 128
NCOL = 256
BR = 64
SLOTS = 192
NB = 2048
BC = 256
N_ROW = 32
N_COL = 8


def pattern(key):
    key_fill = jax.random.fold_in(key, 11)
    key_busy = jax.random.fold_in(key, 12)
    key_rows = jax.random.fold_in(key, 13)
    key_cols = jax.random.fold_in(key, 14)
    filled = SLOTS // 8 + jax.random.randint(key_fill, (N_ROW, N_COL), 0, SLOTS // 4 + 1)
    busiest = jax.random.randint(key_busy, (), 0, N_ROW * N_COL)
    position = jnp.arange(N_ROW * N_COL, dtype=jnp.int32).reshape(N_ROW, N_COL)
    filled = jnp.where(position == busiest, 3 * SLOTS // 4, filled)
    slot_ids = jnp.arange(SLOTS, dtype=jnp.int32)
    rows = jax.random.randint(key_rows, (N_ROW, N_COL, SLOTS), 0, BR)
    rows = jnp.where(slot_ids[None, None, :] < filled[:, :, None], rows, BR)
    bounds = jnp.arange(BR + 1, dtype=jnp.int32)
    pointers = jnp.sum((rows[:, :, None, :] < bounds[None, None, :, None]).astype(jnp.int32), axis=-1)
    group_start = (jnp.arange(N_COL, dtype=jnp.int32) * BC)[None, :, None]
    columns = jax.random.randint(key_cols, (N_ROW, N_COL, SLOTS), 0, BC) + group_start
    return (pointers.astype(jnp.int32), columns.astype(jnp.int32))


def draw_row_ptr(key, part):
    pointers, columns = pattern(key)
    return pointers


def draw_block_cols(key, part):
    pointers, columns = pattern(key)
    return columns


def level_of(rng, shape, pieces, low, top_value):
    gain = 1.0
    for dim, shards_of in pieces:
        heights = jax.random.uniform(jax.random.fold_in(jax.random.fold_in(rng, 6), dim), (shards_of,), jnp.float32, low / len(pieces), top_value / len(pieces))
        gain = gain * jnp.repeat(jnp.exp(heights), shape[dim] // shards_of).reshape((-1,) + (1,) * (len(shape) - 1 - dim))
    return gain


def scatter_about(rng, dims, scale, most, split=(), kind=jnp.bfloat16):
    array = scale * jax.random.normal(rng, dims, jnp.float32)
    if split:
        array = array * level_of(rng, dims, split, -0.22, 0.18)
    return jnp.clip(array, -most, most).astype(kind)


def setup_inputs(seed: int = 0) -> dict:
    seeds = jax.random.split(jax.random.key(seed), 5)
    features = scatter_about(seeds[0], (NB * B, NCOL), 1.0, 6.0, ((0, 256),))
    block_values = scatter_about(seeds[1], (N_ROW, N_COL, SLOTS, B, B), (9 * B) ** -0.5, 0.1875, ((0, 32), (1, 8)))
    row_ptr = draw_row_ptr(jax.random.fold_in(seeds[4], 71), 0)
    block_cols = draw_block_cols(jax.random.fold_in(seeds[4], 71), 0)
    return dict(features=features, block_values=block_values, row_ptr=row_ptr, block_cols=block_cols)


def row_weights(pointers, slot_count):
    slot_ids = jnp.arange(slot_count, dtype=jnp.int32)
    inside = (pointers[:-1, None] <= slot_ids[None, :]) & (slot_ids[None, :] < pointers[1:, None])
    return inside.astype(jnp.float32)


def reference(features, block_values, row_ptr, block_cols):
    block_size = block_values.shape[-1]
    panel = features.reshape(-1, block_size, features.shape[1])

    def one_group(operands):
        values_row, pointers_row, columns_row = operands

        def add_device(running, device_ops):
            values, pointers, columns = device_ops
            blocks = panel[columns.astype(jnp.int32)].astype(jnp.float32)
            products = jnp.einsum("sij,sjk->sik", values.astype(jnp.float32), blocks, precision=lax.Precision.HIGHEST)
            weights = row_weights(pointers.astype(jnp.int32), values.shape[0])
            summed = jnp.einsum("rs,sik->rik", weights, products, precision=lax.Precision.HIGHEST)
            return running + summed, jnp.zeros((), jnp.float32)

        starting = jnp.zeros((row_ptr.shape[2] - 1, block_size, features.shape[1]), jnp.float32)
        running, unused = lax.scan(add_device, starting, (values_row, pointers_row, columns_row))
        return running

    groups = lax.map(one_group, (block_values, row_ptr, block_cols))
    return groups.reshape(features.shape[0], features.shape[1]).astype(jnp.bfloat16)
```

```python
import functools

import jax
import jax.numpy as jnp
from jax import lax
from jax.experimental import pallas as pl
from jax.experimental.pallas import tpu as pltpu
from jax.sharding import PartitionSpec as P

MESH = pl.DeviceIdType.MESH
SIDE = 4
GROUP = 8
ROOM = 144
LIMIT = 32767.0


def gather_kernel(x_ref, out_ref, own, local_sem, send_sem, recv_sem, near_send, near_recv):
    me, col = lax.axis_index("row"), lax.axis_index("col")
    core, x, y = lax.rem(me, 2), lax.rem(me // 2, SIDE), me // (2 * SIDE)
    depth = own.shape[0]
    half, quarter = depth // 2, depth // 4
    sends, slots, near = [], {}, []

    def rank(h, i, j, which):
        dx, dy = (i, j) if h == 0 else (j, i)
        return (lax.rem(y + dy + SIDE, SIDE) * SIDE + lax.rem(x + dx + SIDE, SIDE)) * 2 + which

    def rows(h, part):
        return {
            "all": pl.ds(h * half, half),
            "first": pl.ds(h * half, quarter),
            "second": pl.ds(h * half + quarter, quarter),
        }[part]

    def key(h, i, j, part):
        return (h, (i + 1) % SIDE, (j + 1) % SIDE, part)

    def send(h, i, j, part, di, dj):
        span = rows(h, part)
        dst = out_ref.at[rank(h, i, j, core), span]
        src = own.at[span] if (i, j) == (0, 0) else dst
        k = len(sends)
        copy = pltpu.make_async_remote_copy(
            src_ref=src,
            dst_ref=dst,
            send_sem=send_sem.at[k],
            recv_sem=recv_sem.at[k],
            device_id=(rank(h, di, dj, core), col),
            device_id_type=MESH,
        )
        copy.start()
        sends.append(copy)
        slots[key(h, i - di, j - dj, part)] = k

    def arrive(h, i, j, part):
        k = slots[key(h, i, j, part)]
        span = out_ref.at[rank(h, i, j, core), rows(h, part)]
        pltpu.make_async_remote_copy(
            src_ref=span,
            dst_ref=span,
            send_sem=send_sem.at[k],
            recv_sem=recv_sem.at[k],
            device_id=(me, col),
            device_id_type=MESH,
        ).wait_recv()

    def across(src, dst, other):
        k = len(near)
        copy = pltpu.make_async_remote_copy(
            src_ref=src,
            dst_ref=dst,
            send_sem=near_send.at[k],
            recv_sem=near_recv.at[k],
            device_id=(me + 1 - 2 * core, col),
            device_id_type=MESH,
        )
        copy.start()
        near.append((copy, other))

    def hand_on(h, i, j):
        span = rows(h, "all")
        here = out_ref.at[rank(h, i, j, core), span]
        across(here, here, out_ref.at[rank(h, i, j, 1 - core), span])

    load = pltpu.make_async_copy(x_ref, own, local_sem.at[0])
    load.start()
    barrier = pltpu.get_barrier_semaphore()
    neighbours = [rank(0, 1, 0, core), rank(0, -1, 0, core), rank(0, 0, 1, core), rank(0, 0, -1, core), rank(0, 0, 0, 1 - core)]
    for device in neighbours:
        pl.semaphore_signal(barrier, inc=1, device_id=(device, col), device_id_type=MESH)
    pl.semaphore_wait(barrier, len(neighbours))
    load.wait()

    for h in (0, 1):
        for s in (1, -1):
            send(h, 0, 0, "all", s, 0)
    for h in (0, 1):
        for s in (1, -1):
            send(h, 0, 0, "all", 0, s)
    across(own, out_ref.at[me], out_ref.at[me + 1 - 2 * core])
    keep = pltpu.make_async_copy(own, out_ref.at[me], local_sem.at[1])
    keep.start()
    part_of = {-1: "first", 1: "second"}
    for s in (-1, 1):
        for h in (0, 1):
            arrive(h, s, 0, "all")
            send(h, s, 0, part_of[s], -s, 0)
            send(h, s, 0, "all", 0, 1)
            send(h, s, 0, "all", 0, -1)
            hand_on(h, s, 0)
    for s in (-1, 1):
        for h in (0, 1):
            arrive(h, 0, s, "all")
            send(h, 0, s, part_of[s], 0, -s)
            hand_on(h, 0, s)
    for h in (0, 1):
        for part in ("first", "second"):
            arrive(h, 2, 0, part)
        send(h, 2, 0, "all", 0, 1)
        send(h, 2, 0, "all", 0, -1)
        hand_on(h, 2, 0)
    for i in (-1, 1, 2):
        for s in (-1, 1):
            for h in (0, 1):
                arrive(h, i, s, "all")
                send(h, i, s, part_of[s], 0, -s)
                hand_on(h, i, s)
    for i in (0, -1, 1, 2):
        for h in (0, 1):
            for part in ("first", "second"):
                arrive(h, i, 2, part)
            hand_on(h, i, 2)
    keep.wait()
    for k, (copy, other) in enumerate(near):
        pltpu.make_async_remote_copy(
            src_ref=other,
            dst_ref=other,
            send_sem=near_send.at[k],
            recv_sem=near_recv.at[k],
            device_id=(me + 1 - 2 * core, col),
            device_id_type=MESH,
        ).wait_recv()
    for copy, _ in near:
        copy.wait_send()
    for copy in sends:
        copy.wait_send()


def gather(features, ranks):
    depth, width = features.shape
    links, crossings = 40, 31
    return pl.pallas_call(
        gather_kernel,
        out_shape=jax.ShapeDtypeStruct((ranks, depth, width), features.dtype),
        in_specs=[pl.BlockSpec(memory_space=pl.ANY)],
        out_specs=pl.BlockSpec(memory_space=pl.ANY),
        scratch_shapes=[
            pltpu.VMEM((depth, width), features.dtype),
            pltpu.SemaphoreType.DMA((2,)),
            pltpu.SemaphoreType.DMA((links,)),
            pltpu.SemaphoreType.DMA((links,)),
            pltpu.SemaphoreType.DMA((crossings,)),
            pltpu.SemaphoreType.DMA((crossings,)),
        ],
        compiler_params=pltpu.CompilerParams(collective_id=0, has_side_effects=True),
        name="gather",
    )(features)


def multiply_kernel(ptr_ref, cols_ref, x_ref, a_ref, p_ref, xbuf, abuf, row_of, xsem, asem):
    blocks, side = x_ref.shape[0], x_ref.shape[1]
    local_rows = ptr_ref.shape[0] - 1
    used = ptr_ref[local_rows]
    groups = (used + GROUP - 1) // GROUP

    def values(g):
        span = pl.ds(g * GROUP, GROUP)
        return pltpu.make_async_copy(a_ref.at[span], abuf.at[span], asem.at[g])

    def fetch(g, carry):
        values(g).start()
        for u in range(GROUP):
            s = g * GROUP + u
            pltpu.make_async_copy(x_ref.at[lax.rem(cols_ref[s], blocks)], xbuf.at[s], xsem.at[g]).start()
        return carry

    lax.fori_loop(0, groups, fetch, 0)

    def clear(i, carry):
        p_ref[pl.ds(pl.multiple_of(i * side, side), side), :] = jnp.zeros((side, p_ref.shape[1]), jnp.float32)
        return carry

    lax.fori_loop(0, local_rows, clear, 0)

    def label(i, carry):
        def one(s, c):
            row_of[s] = i
            return c

        return lax.fori_loop(ptr_ref[i], ptr_ref[i + 1], one, carry)

    lax.fori_loop(0, local_rows, label, 0)

    def spare(s, c):
        row_of[s] = local_rows
        return c

    lax.fori_loop(used, groups * GROUP, spare, 0)

    def step(g, carry):
        values(g).wait()
        span = pl.ds(g * GROUP, GROUP)
        pltpu.make_async_copy(x_ref.at[pl.ds(0, GROUP)], xbuf.at[span], xsem.at[g]).wait()
        for u in range(GROUP):
            s = g * GROUP + u
            product = jnp.dot(abuf[s], xbuf[s], preferred_element_type=jnp.float32)
            place = pl.ds(pl.multiple_of(row_of[s] * side, side), side)
            p_ref[place, :] += product
        return carry

    lax.fori_loop(0, groups, step, 0)


def multiply(pointers, columns, panel, values):
    side, width = panel.shape[1], panel.shape[2]
    local_rows = pointers.shape[0] - 1
    return pl.pallas_call(
        multiply_kernel,
        out_shape=jax.ShapeDtypeStruct(((local_rows + 1) * side, width), jnp.float32),
        in_specs=[
            pl.BlockSpec(memory_space=pltpu.SMEM),
            pl.BlockSpec(memory_space=pltpu.SMEM),
            pl.BlockSpec(memory_space=pl.ANY),
            pl.BlockSpec(memory_space=pl.ANY),
        ],
        out_specs=pl.BlockSpec(memory_space=pltpu.VMEM),
        scratch_shapes=[
            pltpu.VMEM((ROOM, side, width), jnp.bfloat16),
            pltpu.VMEM((ROOM, side, side), jnp.bfloat16),
            pltpu.SMEM((ROOM,), jnp.int32),
            pltpu.SemaphoreType.DMA((ROOM // GROUP,)),
            pltpu.SemaphoreType.DMA((ROOM // GROUP,)),
        ],
        compiler_params=pltpu.CompilerParams(vmem_limit_bytes=30 * 1024 * 1024),
        name="multiply",
    )(pointers, columns, panel, values)


def reduce_kernel(
    side, p_ref, o_ref, part, sent, got, sent_scale, got_scale, load_sem, send_sem, recv_sem, scale_send, scale_recv
):
    row, me = lax.axis_index("row"), lax.axis_index("col")
    ring = lax.axis_size("col")
    depth, width = o_ref.shape
    lanes = width // 2
    far = ring // 2

    def at(offset):
        return lax.rem(me + offset + ring, ring)

    order = [far] + [s * t for t in range(far - 1, 0, -1) for s in (1, -1)] + [0]
    place = {offset: n for n, offset in enumerate(order)}
    place[-far] = place[far]
    loads = {}
    for n, offset in enumerate(order):
        loads[n] = pltpu.make_async_copy(
            p_ref.at[pl.ds(pl.multiple_of(at(offset) * depth, depth), depth)], part.at[n], load_sem.at[n]
        )
        loads[n].start()

    barrier = pltpu.get_barrier_semaphore()
    for s in (1, -1):
        pl.semaphore_signal(barrier, inc=1, device_id=(row, at(s)), device_id_type=MESH)
    pl.semaphore_wait(barrier, 2)

    def copies(w, k, s):
        return [
            pltpu.make_async_remote_copy(
                src_ref=a.at[w, k],
                dst_ref=b.at[w, k],
                send_sem=c.at[w, k],
                recv_sem=d.at[w, k],
                device_id=(row, at(s)),
                device_id_type=MESH,
            )
            for a, b, c, d in ((sent, got, send_sem, recv_sem), (sent_scale, got_scale, scale_send, scale_recv))
        ]

    def spread(w, k, j):
        return got[w, k, pl.ds(pl.multiple_of(j * side, side), side), :].astype(jnp.int32).astype(jnp.float32) * got_scale[
            w, k, pl.ds(j, 1), :
        ]

    def columns(w, k):
        h = w if k % 2 == 0 else 1 - w
        return pl.ds(h * lanes, lanes)

    loaded = set()

    def need(n):
        if n not in loaded:
            loaded.add(n)
            loads[n].wait()

    started = []
    for k in range(ring - 1):
        for w, s in ((0, 1), (1, -1)):
            n = place[s * (far - (k + 1) // 2)]
            need(n)
            if k >= 2:
                for copy in copies(w, k - 2, s):
                    copy.wait_recv()

            def code(j, carry, w=w, k=k, n=n):
                span = pl.ds(pl.multiple_of(j * side, side), side)
                value = part[n, span, columns(w, k)]
                if k >= 2:
                    value = value + spread(w, k - 2, j)
                top = jnp.maximum(jnp.max(jnp.abs(value), axis=0, keepdims=True), 1e-30)
                sent_scale[w, k, pl.ds(j, 1), :] = top * (1.0 / LIMIT)
                sent[w, k, span, :] = jnp.round(value * (LIMIT / top)).astype(jnp.int32).astype(jnp.int16)
                return carry

            lax.fori_loop(0, depth // side, code, 0)
            for copy in copies(w, k, s):
                copy.start()
                started.append(copy)

    need(place[0])
    for w, s in ((0, 1), (1, -1)):
        for k in (ring - 3, ring - 2):
            for copy in copies(w, k, s):
                copy.wait_recv()

    def finish(j, carry):
        span = pl.ds(pl.multiple_of(j * side, side), side)
        for h in (0, 1):
            cut = pl.ds(h * lanes, lanes)
            value = part[place[0], span, cut] + (spread(h, ring - 2, j) + spread(1 - h, ring - 3, j))
            o_ref[span, cut] = value.astype(o_ref.dtype)
        return carry

    lax.fori_loop(0, depth // side, finish, 0)
    for copy in started:
        copy.wait_send()


def reduce(partial_value, side, ring, depth):
    width = partial_value.shape[1]
    steps = ring - 1
    return pl.pallas_call(
        functools.partial(reduce_kernel, side),
        out_shape=jax.ShapeDtypeStruct((depth, width), jnp.bfloat16),
        in_specs=[pl.BlockSpec(memory_space=pl.ANY)],
        out_specs=pl.BlockSpec(memory_space=pltpu.VMEM),
        scratch_shapes=[
            pltpu.VMEM((ring, depth, width), jnp.float32),
            pltpu.VMEM((2, steps, depth, width // 2), jnp.int16),
            pltpu.VMEM((2, steps, depth, width // 2), jnp.int16),
            pltpu.VMEM((2, steps, depth // side, width // 2), jnp.float32),
            pltpu.VMEM((2, steps, depth // side, width // 2), jnp.float32),
            pltpu.SemaphoreType.DMA((ring,)),
            pltpu.SemaphoreType.DMA((2, steps)),
            pltpu.SemaphoreType.DMA((2, steps)),
            pltpu.SemaphoreType.DMA((2, steps)),
            pltpu.SemaphoreType.DMA((2, steps)),
        ],
        compiler_params=pltpu.CompilerParams(
            collective_id=1, has_side_effects=True, vmem_limit_bytes=20 * 1024 * 1024
        ),
        name="reduce",
    )(partial_value)


def local(features, block_values, row_ptr, block_cols):
    values, pointers, columns = block_values[0, 0], row_ptr[0, 0], block_cols[0, 0]
    side = values.shape[1]
    ranks, ring = lax.axis_size("row"), lax.axis_size("col")
    panel = gather(features, ranks)
    panel = panel.reshape(ranks * features.shape[0] // side, side, features.shape[1])
    partial_value = multiply(pointers, columns, panel, values)
    return reduce(partial_value, side, ring, (pointers.shape[0] - 1) * side // ring)


def solution(mesh):
    return jax.shard_map(
        local,
        mesh=mesh,
        in_specs=(
            P(("col", "row"), None),
            P("row", "col", None, None, None),
            P("row", "col", None),
            P("row", "col", None),
        ),
        out_specs=P(("row", "col"), None),
        check_vma=False,
    )
```

```python
import jax
import jax.numpy as jnp
from jax import lax
from jax.experimental import pallas as pl
from jax.experimental.pallas import tpu as pltpu
from jax.sharding import PartitionSpec as P

MESH = pl.DeviceIdType.MESH
SIDE = 4
GROUP = 8
ROOM = 144
LIMIT = 32767.0
LINKS, CROSSINGS = 40, 31


class Gather:
    def __init__(self, c, panels, send_sem, recv_sem, near_send, near_recv):
        me, self.col = lax.axis_index("row"), lax.axis_index("col")
        self.c, self.panel = c, panels[c]
        self.core, self.x, self.y = lax.rem(me, 2), lax.rem(me // 2, SIDE), me // (2 * SIDE)
        self.depth = self.panel.shape[0] // lax.axis_size("row")
        self.send_sem, self.recv_sem, self.near_send, self.near_recv = send_sem, recv_sem, near_send, near_recv
        self.sends, self.slots, self.near = [], {}, []

    def rank(self, h, i, j, other=False):
        dx, dy = (i, j) if h == 0 else (j, i)
        core = 1 - self.core if other else self.core
        return (lax.rem(self.y + dy + SIDE, SIDE) * SIDE + lax.rem(self.x + dx + SIDE, SIDE)) * 2 + core

    def piece(self, h, i, j, part, other=False):
        half, quarter = self.depth // 2, self.depth // 4
        first, size = {"all": (0, half), "first": (0, quarter), "second": (quarter, quarter)}[part]
        return self.panel.at[pl.ds(self.rank(h, i, j, other) * self.depth + h * half + first, size)]

    def key(self, h, i, j, part):
        return (h, (i + 1) % SIDE, (j + 1) % SIDE, part)

    def link(self, k, ref, device):
        return pltpu.make_async_remote_copy(
            src_ref=ref,
            dst_ref=ref,
            send_sem=self.send_sem.at[self.c, k],
            recv_sem=self.recv_sem.at[self.c, k],
            device_id=(device, self.col),
            device_id_type=MESH,
        )

    def across(self, k, ref):
        return pltpu.make_async_remote_copy(
            src_ref=ref,
            dst_ref=ref,
            send_sem=self.near_send.at[self.c, k],
            recv_sem=self.near_recv.at[self.c, k],
            device_id=(self.rank(0, 0, 0, True), self.col),
            device_id_type=MESH,
        )

    def send(self, h, i, j, part, di, dj):
        k = len(self.sends)
        copy = self.link(k, self.piece(h, i, j, part), self.rank(h, di, dj))
        copy.start()
        self.sends.append(copy)
        self.slots[self.key(h, i - di, j - dj, part)] = k

    def arrive(self, h, i, j, part):
        self.link(self.slots[self.key(h, i, j, part)], self.piece(h, i, j, part), self.rank(h, 1, 0)).wait_recv()

    def hand_on(self, h, i, j):
        k = len(self.near)
        copy = self.across(k, self.piece(h, i, j, "all"))
        copy.start()
        self.near.append((copy, self.across(k, self.piece(h, i, j, "all", True))))

    def own(self):
        for di, dj in ((1, 0), (-1, 0), (0, 1), (0, -1)):
            for h in (0, 1):
                self.send(h, 0, 0, "all", di, dj)
        k = len(self.near)
        refs = [self.panel.at[pl.ds(self.rank(0, 0, 0, o) * self.depth, self.depth)] for o in (False, True)]
        copy = self.across(k, refs[0])
        copy.start()
        self.near.append((copy, self.across(k, refs[1])))

    def forward(self, h, i, j):
        self.send(h, i, j, "first" if j == -1 else "second", 0, -j)

    def first_hop(self):
        for s in (-1, 1):
            for h in (0, 1):
                self.arrive(h, s, 0, "all")
                self.send(h, s, 0, "first" if s == -1 else "second", -s, 0)
                self.send(h, s, 0, "all", 0, 1)
                self.send(h, s, 0, "all", 0, -1)
                self.hand_on(h, s, 0)

    def second_hop(self):
        for h in (0, 1):
            for part in ("first", "second"):
                self.arrive(h, 2, 0, part)
            self.send(h, 2, 0, "all", 0, 1)
            self.send(h, 2, 0, "all", 0, -1)
            self.hand_on(h, 2, 0)

    def turn(self, i):
        for s in (-1, 1):
            for h in (0, 1):
                self.arrive(h, i, s, "all")
                self.forward(h, i, s)
                self.hand_on(h, i, s)

    def last(self, i):
        for h in (0, 1):
            for part in ("first", "second"):
                self.arrive(h, i, 2, part)
            self.hand_on(h, i, 2)

    def all_here(self):
        for _, coming in self.near:
            coming.wait_recv()

    def drain(self):
        for copy in self.sends:
            copy.wait_send()
        for copy, _ in self.near:
            copy.wait_send()


class Reduce:
    def __init__(self, c, ptr, run, o_ref, sent, got, sent_scale, got_scale, sems):
        self.row, self.me, self.ring = lax.axis_index("row"), lax.axis_index("col"), lax.axis_size("col")
        self.c, self.ptr, self.run, self.o_ref = c, ptr, run, o_ref
        self.sent, self.got, self.sent_scale, self.got_scale, self.sems = sent, got, sent_scale, got_scale, sems
        self.side = run.shape[2]
        self.blocks = o_ref.shape[0] // self.side
        self.started = []

    def at(self, offset):
        return lax.rem(self.me + offset + self.ring, self.ring)

    def copies(self, w, k):
        send_sem, recv_sem, scale_send, scale_recv = self.sems
        c = self.c
        return [
            pltpu.make_async_remote_copy(
                src_ref=a.at[c, w, k],
                dst_ref=b.at[c, w, k],
                send_sem=s.at[c, w, k],
                recv_sem=r.at[c, w, k],
                device_id=(self.row, self.at(1 - 2 * w)),
                device_id_type=MESH,
            )
            for a, b, s, r in (
                (self.sent, self.got, send_sem, recv_sem),
                (self.sent_scale, self.got_scale, scale_send, scale_recv),
            )
        ]

    def partial(self, offset, h, j):
        i = self.at(offset) * self.blocks + h * (self.blocks // 2) + j
        end = self.ptr[i + 1]
        return self.run[self.c, jnp.where(end > self.ptr[i], end, 0)]

    def spread(self, w, k, j):
        span = pl.ds(pl.multiple_of(j * self.side, self.side), self.side)
        return self.got[self.c, w, k, span, :].astype(jnp.int32).astype(jnp.float32) * self.got_scale[self.c, w, k, pl.ds(j, 1), :]

    def step(self, k):
        for w in (0, 1):
            offset, h = (1 - 2 * w) * (self.ring // 2 - (k + 1) // 2), w if k % 2 == 0 else 1 - w
            if k >= 2:
                for copy in self.copies(w, k - 2):
                    copy.wait_recv()

            def code(j, carry, w=w, offset=offset, h=h):
                value = self.partial(offset, h, j)
                if k >= 2:
                    value = value + self.spread(w, k - 2, j)
                top = jnp.maximum(jnp.max(jnp.abs(value), axis=0, keepdims=True), 1e-30)
                self.sent_scale[self.c, w, k, pl.ds(j, 1), :] = top * (1.0 / LIMIT)
                span = pl.ds(pl.multiple_of(j * self.side, self.side), self.side)
                self.sent[self.c, w, k, span, :] = jnp.round(value * (LIMIT / top)).astype(jnp.int32).astype(jnp.int16)
                return carry

            lax.fori_loop(0, self.blocks // 2, code, 0)
            for copy in self.copies(w, k):
                copy.start()
                self.started.append(copy)

    def finish(self):
        last = self.ring - 2
        for k in (last - 1, last):
            for w in (0, 1):
                for copy in self.copies(w, k):
                    copy.wait_recv()
        lanes = self.run.shape[3]
        for h in (0, 1):

            def add(j, carry, h=h):
                value = self.partial(0, h, j) + (self.spread(h, last, j) + self.spread(1 - h, last - 1, j))
                start = (h * (self.blocks // 2) + j) * self.side
                span = pl.ds(pl.multiple_of(start, self.side), self.side)
                self.o_ref[span, pl.ds(self.c * lanes, lanes)] = value.astype(self.o_ref.dtype)
                return carry

            lax.fori_loop(0, self.blocks // 2, add, 0)

    def drain(self):
        for copy in self.started:
            copy.wait_send()


def kernel(
    ptr, cols, ptr_row, x_ref, a_ref, o_ref,
    panel_one, panel_two, values, run, same, sent, got, sent_scale, got_scale,
    load_sem, link_send, link_recv, near_send, near_recv, send_sem, recv_sem, scale_send, scale_recv,
):
    row, col = lax.axis_index("row"), lax.axis_index("col")
    panels = (panel_one, panel_two)
    blocks, side, lanes = panel_one.shape
    depth = blocks // lax.axis_size("row")

    loads = [
        pltpu.make_async_copy(
            x_ref.at[:, :, pl.ds(c * lanes, lanes)], panels[c].at[pl.ds(row * depth, depth)], load_sem.at[c]
        )
        for c in (0, 1)
    ] + [pltpu.make_async_copy(a_ref.at[pl.ds(0, ROOM)], values, load_sem.at[2])]
    for load in loads:
        load.start()

    gathers = [Gather(c, panels, link_send, link_recv, near_send, near_recv) for c in (0, 1)]
    sems = (send_sem, recv_sem, scale_send, scale_recv)
    sums = [Reduce(c, ptr, run, o_ref, sent, got, sent_scale, got_scale, sems) for c in (0, 1)]
    g, r = gathers[0], sums[0]
    barrier = pltpu.get_barrier_semaphore()
    neighbours = [(g.rank(0, i, j), col) for i, j in ((1, 0), (-1, 0), (0, 1), (0, -1))]
    neighbours += [(g.rank(0, 0, 0, True), col), (row, r.at(1)), (row, r.at(-1))]
    for device in neighbours:
        pl.semaphore_signal(barrier, inc=1, device_id=device, device_id_type=MESH)
    pl.semaphore_wait(barrier, len(neighbours))

    def multiply(c, first, last):
        def step(n, carry):
            total = run[c, n * GROUP]
            for u in range(GROUP):
                s = n * GROUP + u
                product = jnp.dot(values[s], panels[c][lax.rem(cols[s], blocks)], preferred_element_type=jnp.float32)
                total = total * same[pl.ds(s, 1), :] + product
                run[c, s + 1] = total
            return carry

        lax.fori_loop(first, last, step, 0)

    halfway, whole = ROOM // GROUP // 2, ROOM // GROUP
    one, two = gathers
    sum1, sum2 = sums

    loads[0].wait()
    one.own()
    loads[1].wait()
    starts = jnp.max(
        (lax.broadcasted_iota(jnp.int32, (ROOM, ptr_row.shape[1]), 0) == ptr_row[...]).astype(jnp.float32), axis=1, keepdims=True
    )
    same[...] = jnp.broadcast_to(1.0 - starts, same.shape)
    for c in (0, 1):
        run[c, 0] = jnp.zeros((side, lanes), jnp.float32)
    loads[2].wait()
    one.first_hop()
    one.turn(0)
    one.second_hop()
    one.turn(-1)
    one.turn(1)
    one.turn(2)
    two.own()
    for i in (0, -1, 1, 2):
        one.last(i)
    one.all_here()
    multiply(0, 0, halfway)
    two.first_hop()
    multiply(0, halfway, whole)
    sum1.step(0)
    sum1.step(1)
    two.turn(0)
    two.second_hop()
    two.turn(-1)
    sum1.step(2)
    two.turn(1)
    sum1.step(3)
    sum1.step(4)
    two.turn(2)
    for i in (0, -1, 1):
        two.last(i)
    sum1.step(5)
    two.last(2)
    two.all_here()
    multiply(1, 0, halfway)
    sum1.step(6)
    multiply(1, halfway, whole)
    sum2.step(0)
    sum2.step(1)
    sum1.finish()
    for k in range(2, 7):
        sum2.step(k)
    sum2.finish()
    for stream in (*gathers, *sums):
        stream.drain()


def local(features, block_values, row_ptr, block_cols):
    values, pointers, columns = block_values[0, 0], row_ptr[0, 0], block_cols[0, 0]
    side = values.shape[1]
    ranks, ring = lax.axis_size("row"), lax.axis_size("col")
    depth, width = features.shape
    lanes = width // 2
    blocks = ranks * depth // side
    owned = (pointers.shape[0] - 1) * side // ring
    steps = ring - 1
    return pl.pallas_call(
        kernel,
        out_shape=jax.ShapeDtypeStruct((owned, width), jnp.bfloat16),
        in_specs=[
            pl.BlockSpec(memory_space=pltpu.SMEM),
            pl.BlockSpec(memory_space=pltpu.SMEM),
            pl.BlockSpec(memory_space=pltpu.VMEM),
            pl.BlockSpec(memory_space=pl.ANY),
            pl.BlockSpec(memory_space=pl.ANY),
        ],
        out_specs=pl.BlockSpec(memory_space=pltpu.VMEM),
        scratch_shapes=[
            pltpu.VMEM((blocks, side, lanes), jnp.bfloat16),
            pltpu.VMEM((blocks, side, lanes), jnp.bfloat16),
            pltpu.VMEM((ROOM, side, side), jnp.bfloat16),
            pltpu.VMEM((2, ROOM + 1, side, lanes), jnp.float32),
            pltpu.VMEM((ROOM, lanes), jnp.float32),
            pltpu.VMEM((2, 2, steps, owned // 2, lanes), jnp.int16),
            pltpu.VMEM((2, 2, steps, owned // 2, lanes), jnp.int16),
            pltpu.VMEM((2, 2, steps, owned // side // 2, lanes), jnp.float32),
            pltpu.VMEM((2, 2, steps, owned // side // 2, lanes), jnp.float32),
            pltpu.SemaphoreType.DMA((3,)),
            pltpu.SemaphoreType.DMA((2, LINKS)),
            pltpu.SemaphoreType.DMA((2, LINKS)),
            pltpu.SemaphoreType.DMA((2, CROSSINGS)),
            pltpu.SemaphoreType.DMA((2, CROSSINGS)),
            pltpu.SemaphoreType.DMA((2, 2, steps)),
            pltpu.SemaphoreType.DMA((2, 2, steps)),
            pltpu.SemaphoreType.DMA((2, 2, steps)),
            pltpu.SemaphoreType.DMA((2, 2, steps)),
        ],
        compiler_params=pltpu.CompilerParams(
            collective_id=0, has_side_effects=True, vmem_limit_bytes=60 * 1024 * 1024
        ),
        name="block_sparse",
    )(pointers, columns, pointers[None, :], features.reshape(depth // side, side, width), values)


def solution(mesh):
    return jax.shard_map(
        local,
        mesh=mesh,
        in_specs=(
            P(("col", "row"), None),
            P("row", "col", None, None, None),
            P("row", "col", None),
            P("row", "col", None),
        ),
        out_specs=P(("row", "col"), None),
        check_vma=False,
    )
```

```python
import jax
import jax.numpy as jnp
from jax import lax
from jax.experimental import pallas as pl
from jax.experimental.pallas import tpu as pltpu
from jax.sharding import PartitionSpec as P

MESH = pl.DeviceIdType.MESH
SIDE = 4
GROUP = 8
ROOM = 144
LIMIT = 32767.0
CHUNKS = 4
EVENTS = 10
PARTS = 6
SUMS = 3


class Gather:
    def __init__(self, c, panels, send_sem, recv_sem, near_recv):
        me, self.col = lax.axis_index("row"), lax.axis_index("col")
        self.c, self.panel = c, panels[c]
        self.core, self.x, self.y = lax.rem(me, 2), lax.rem(me // 2, SIDE), me // (2 * SIDE)
        self.depth = self.panel.shape[0] // lax.axis_size("row")
        self.send_sem, self.recv_sem, self.near_recv = send_sem.at[c], recv_sem, near_recv.at[c]
        self.sent, self.due, self.near = 0, [0] * EVENTS, 0

    def rank(self, h, i, j, other=False):
        dx, dy = (i, j) if h == 0 else (j, i)
        core = 1 - self.core if other else self.core
        return (lax.rem(self.y + dy + SIDE, SIDE) * SIDE + lax.rem(self.x + dx + SIDE, SIDE)) * 2 + core

    def piece(self, h, i, j, part, other=False):
        half, quarter = self.depth // 2, self.depth // 4
        first, size = {"all": (0, half), "first": (0, quarter), "second": (quarter, quarter)}[part]
        return self.panel.at[pl.ds(self.rank(h, i, j, other) * self.depth + h * half + first, size)]

    def event(self, i, j):
        i, j = (i + 1) % SIDE - 1, (j + 1) % SIDE - 1
        return {0: 0 if i != 2 else 1, 2: 6 + i + 1}.get(j, 2 + i + 1)

    def start(self, ref, recv_sem, device):
        pltpu.make_async_remote_copy(
            src_ref=ref,
            dst_ref=ref,
            send_sem=self.send_sem,
            recv_sem=recv_sem,
            device_id=(device, self.col),
            device_id_type=MESH,
        ).start()
        self.sent += ref.shape[0]
        return ref.shape[0]

    def blocks(self, count, recv_sem):
        ref = self.panel.at[pl.ds(0, count)]
        return pltpu.make_async_remote_copy(
            src_ref=ref,
            dst_ref=ref,
            send_sem=self.send_sem,
            recv_sem=recv_sem,
            device_id=(self.rank(0, 0, 0, True), self.col),
            device_id_type=MESH,
        )

    def send(self, h, i, j, part, di, dj):
        event = self.event(i - di, j - dj)
        self.due[event] += self.start(self.piece(h, i, j, part), self.recv_sem.at[self.c, event], self.rank(h, di, dj))

    def arrive(self, i, j):
        event = self.event(i, j)
        self.blocks(self.due[event], self.recv_sem.at[self.c, event]).wait_recv()

    def hand_on(self, h, i, j):
        self.near += self.start(self.piece(h, i, j, "all"), self.near_recv, self.rank(0, 0, 0, True))

    def own(self):
        for di, dj in ((1, 0), (-1, 0), (0, 1), (0, -1)):
            for h in (0, 1):
                self.send(h, 0, 0, "all", di, dj)
        mine = self.panel.at[pl.ds(self.rank(0, 0, 0) * self.depth, self.depth)]
        self.near += self.start(mine, self.near_recv, self.rank(0, 0, 0, True))

    def forward(self, h, i, j):
        self.send(h, i, j, "first" if j == -1 else "second", 0, -j)

    def first_hop(self):
        pieces = [(h, s) for s in (-1, 1) for h in (0, 1)]
        self.arrive(1, 0)
        for h, s in pieces:
            self.send(h, s, 0, "first" if s == -1 else "second", -s, 0)
        for h, s in pieces:
            self.send(h, s, 0, "all", 0, 1)
            self.send(h, s, 0, "all", 0, -1)
        for h, s in pieces:
            self.hand_on(h, s, 0)

    def second_hop(self):
        self.arrive(2, 0)
        for h in (0, 1):
            self.send(h, 2, 0, "all", 0, 1)
            self.send(h, 2, 0, "all", 0, -1)
            self.hand_on(h, 2, 0)

    def turn(self, i):
        self.arrive(i, 1)
        for s in (-1, 1):
            for h in (0, 1):
                self.forward(h, i, s)
        for s in (-1, 1):
            for h in (0, 1):
                self.hand_on(h, i, s)

    def last(self, i):
        self.arrive(i, 2)
        for h in (0, 1):
            self.hand_on(h, i, 2)

    def tail(self):
        for i in (0, -1, 1, 2):
            self.last(i)

    def all_here(self):
        self.blocks(self.near, self.near_recv).wait_recv()

    def drain(self):
        self.blocks(self.sent, self.near_recv).wait_send()


class Reduce:
    def __init__(self, c, ptr, run, o_ref, held, sent, got, sent_scale, got_scale, sems):
        self.row, self.me, self.ring = lax.axis_index("row"), lax.axis_index("col"), lax.axis_size("col")
        self.c, self.ptr, self.run, self.o_ref, self.held = c, ptr, run, o_ref, held
        self.sent, self.got, self.sent_scale, self.got_scale, self.sems = sent, got, sent_scale, got_scale, sems
        self.side, self.lanes = run.shape[2:]
        self.pairs = o_ref.shape[0] // self.side // 2
        self.low = lax.broadcasted_iota(jnp.int32, (self.side, self.lanes), 1) < self.lanes // 2

    def at(self, offset):
        return lax.rem(self.me + offset + self.ring, self.ring)

    def copies(self, w, *refs_and_sems):
        for a, b, s, r in refs_and_sems:
            yield pltpu.make_async_remote_copy(
                src_ref=a,
                dst_ref=b,
                send_sem=s,
                recv_sem=r,
                device_id=(self.row, self.at(1 - 2 * w)),
                device_id_type=MESH,
            )

    def both(self, at, k, j=0):
        send_sem, recv_sem, scale_send, scale_recv = self.sems
        at = (self.c, *at)
        r = self.c + j
        return (
            (self.sent.at[at], self.got.at[at], send_sem.at[self.c], recv_sem.at[r, k]),
            (self.sent_scale.at[at], self.got_scale.at[at], scale_send.at[self.c], scale_recv.at[r, k]),
        )

    def arrive(self, k, j=None):
        at = (0, pl.ds(0, 2)) if j is None else (0, 0)
        for copy in self.copies(0, *self.both(at, k, j or 0)):
            copy.wait_recv()

    def total(self, i):
        end = self.ptr[i + 1]
        return self.run[self.c % SUMS, jnp.where(end > self.ptr[i], end, 0)]

    def partial(self, offset, h, j):
        i = (self.at(offset) * self.pairs + h * (self.pairs // 2) + j) * 2
        one, two = self.total(i), self.total(i + 1)
        return jnp.where(self.low, one, two) + self.swap(jnp.where(self.low, two, one))

    def swap(self, value):
        return pltpu.roll(value, self.lanes // 2, 1)

    def spread(self, w, k, j):
        return self.got[self.c, w, k, j].astype(jnp.int32).astype(jnp.float32) * self.got_scale[self.c, w, k, j]

    def encode(self, k, j):
        for w in (0, 1):
            offset, h = (1 - 2 * w) * (self.ring // 2 - (k + 1) // 2), w if k % 2 == 0 else 1 - w
            value = self.partial(offset, h, j)
            if k >= 2:
                value = value + self.spread(w, k - 2, j)
            top = jnp.maximum(jnp.max(jnp.abs(value), axis=0, keepdims=True), 1e-30)
            self.sent_scale[self.c, w, k, j] = top * (1.0 / LIMIT)
            self.sent[self.c, w, k, j] = jnp.round(value * (LIMIT / top)).astype(jnp.int32).astype(jnp.int16)

    def start(self, k, j=None):
        for w in (0, 1):
            for copy in self.copies(w, *self.both((w, k) if j is None else (w, k, j), k, j or 0)):
                copy.start()

    def step(self, k):
        if k >= 2:
            self.arrive(k - 2)
        for j in range(self.pairs // 2):
            self.encode(k, j)
        self.start(k)

    def half_step(self, k):
        for j in range(self.pairs // 2):
            if k >= 2:
                self.arrive(k - 2, j)
            self.encode(k, j)
            self.start(k, j)

    def finish(self, halves=False):
        last = self.ring - 2
        if not halves:
            self.arrive(last - 1)
            self.arrive(last)
        for j in range(self.pairs // 2):
            if halves:
                self.arrive(last - 1, j)
                self.arrive(last, j)
            for h in (0, 1):
                value = self.partial(0, h, j) + (self.spread(h, last, j) + self.spread(1 - h, last - 1, j))
                n = h * (self.pairs // 2) + j
                if self.c % 2 == 0:
                    self.held[n] = value
                else:
                    before = self.held[n]
                    both = jnp.where(self.low, before, self.swap(value)), jnp.where(self.low, self.swap(before), value)
                    for u in (0, 1):
                        span = pl.ds((2 * n + u) * self.side, self.side)
                        self.o_ref[span, pl.ds(self.c // 2 * self.lanes, self.lanes)] = both[u].astype(self.o_ref.dtype)

    def drain(self):
        for copy in self.copies(0, *self.both((), 0)):
            copy.wait_send()


def kernel(
    ptr_ref, cols_ref, ptr_row_ref, cols_row_ref, x_ref, a_ref, o_ref,
    ptr, cols, ptr_row, cols_row, panel_0, panel_1, panel_2, panel_3, own, values, run, same, mine, held, sent, got, sent_scale, got_scale,
    load_sem, link_send, link_recv, near_recv, send_sem, recv_sem, scale_send, scale_recv,
):
    row, col = lax.axis_index("row"), lax.axis_index("col")
    panels = (panel_0, panel_1, panel_2, panel_3)
    pairs, side, lanes = panel_0.shape
    depth = pairs // lax.axis_size("row")

    load = pltpu.make_async_copy(x_ref, own, load_sem.at[0])
    load_values = pltpu.make_async_copy(a_ref.at[pl.ds(0, ROOM)], values, load_sem.at[1])
    small = [
        pltpu.make_async_copy(a, b, load_sem.at[2 + n])
        for n, (a, b) in enumerate(((ptr_ref, ptr), (cols_ref, cols), (ptr_row_ref, ptr_row), (cols_row_ref, cols_row)))
    ]
    for copy in (load, *small, load_values):
        copy.start()

    gathers = [Gather(c, panels, link_send, link_recv, near_recv) for c in range(CHUNKS)]
    sems = (send_sem, recv_sem, scale_send, scale_recv)
    sums = [Reduce(c, ptr, run, o_ref, held, sent, got, sent_scale, got_scale, sems) for c in range(CHUNKS)]
    g, r = gathers[0], sums[0]
    barrier = pltpu.get_barrier_semaphore()
    neighbours = [(g.rank(0, i, j), col) for i, j in ((1, 0), (-1, 0), (0, 1), (0, -1))]
    neighbours += [(g.rank(0, 0, 0, True), col), (row, r.at(1)), (row, r.at(-1))]
    for device in neighbours:
        pl.semaphore_signal(barrier, inc=1, device_id=device, device_id_type=MESH)

    def pack(c):
        for n in range(depth):
            cut = pl.ds(c // 2 * lanes, lanes)
            one, two = (own[2 * n + u, :, cut].astype(jnp.float32) for u in (0, 1))
            if c % 2 == 0:
                two = r.swap(two)
            else:
                one = r.swap(one)
            panels[c][row * depth + n] = jnp.where(r.low, one, two).astype(jnp.bfloat16)

    load.wait()
    pack(0)
    pl.semaphore_wait(barrier, len(neighbours))
    gathers[0].own()
    for c in range(1, CHUNKS):
        pack(c)
    for copy in small:
        copy.wait()
    shape = (ROOM, ptr_row.shape[1])
    starts = jnp.max((lax.broadcasted_iota(jnp.int32, shape, 0) == ptr_row[...]).astype(jnp.float32), axis=1, keepdims=True)
    same[...] = jnp.broadcast_to(1.0 - starts, same.shape)
    shape = (ROOM, cols_row.shape[1])
    slot = lax.broadcasted_iota(jnp.int32, shape, 0) == lax.broadcasted_iota(jnp.int32, shape, 1)
    odd = jnp.max(jnp.where(slot, lax.rem(cols_row[...], 2), 0).astype(jnp.float32), axis=1, keepdims=True)
    high = (lax.broadcasted_iota(jnp.int32, mine.shape, 1) >= lanes // 2).astype(jnp.float32)
    mine[...] = high * odd + (1.0 - high) * (1.0 - odd)
    for n in range(SUMS):
        run[n, 0] = jnp.zeros((side, lanes), jnp.float32)

    def multiply(c, first, last):
        def step(n, carry):
            total = run[c % SUMS, n * GROUP]
            for u in range(GROUP):
                s = n * GROUP + u
                pair = lax.div(lax.rem(cols[s], 2 * pairs), 2)
                product = jnp.dot(values[s], panels[c][pair], preferred_element_type=jnp.float32)
                total = total * same[pl.ds(s, 1), :] + product * mine[pl.ds(s, 1), :]
                run[c % SUMS, s + 1] = total
            return carry

        lax.fori_loop(first, last, step, 0)

    share = ROOM // GROUP // PARTS

    def work(c, *parts):
        for part in parts:
            multiply(c, part * share, (part + 1) * share)

    def take(n, *names):
        for name in names:
            if isinstance(name, int):
                gathers[n].turn(name)
            else:
                getattr(gathers[n], name)()

    def add(n, *steps):
        for k in steps:
            sums[n].step(k)

    load_values.wait()
    take(0, "first_hop", 0, "second_hop")
    take(1, "own")
    take(0, -1, 1, 2)
    take(1, "first_hop", 0)
    take(0, "tail")
    take(1, "second_hop")
    take(2, "own")
    take(0, "all_here")
    work(0, 0)
    take(1, -1)
    work(0, 1)
    take(1, 1)
    work(0, 2, 3)
    take(1, 2)
    work(0, 4)
    take(2, "first_hop")
    work(0, 5)
    add(0, 0, 1)
    take(2, 0)
    take(1, "tail")
    take(2, "second_hop")
    take(3, "own")
    add(0, 2)
    take(1, "all_here")
    work(1, 0)
    take(2, -1)
    add(0, 3)
    work(1, 1)
    take(2, 1)
    work(1, 2, 3)
    take(2, 2)
    work(1, 4)
    add(0, 4)
    work(1, 5)
    take(3, "first_hop")
    add(0, 5)
    add(1, 0, 1)
    take(3, 0)
    take(2, "tail")
    take(3, "second_hop")
    add(0, 6)
    take(2, "all_here")
    take(3, -1)
    work(2, 0)
    take(3, 1)
    add(1, 2)
    work(2, 1)
    add(1, 3)
    work(2, 2)
    take(3, 2)
    work(2, 3)
    sums[0].finish()
    work(2, 4)
    add(1, 4)
    work(2, 5)
    add(2, 0, 1)
    add(1, 5)
    take(3, "tail", "all_here")
    work(3, 0)
    add(1, 6)
    work(3, 1)
    add(2, 2)
    work(3, 2)
    add(2, 3)
    work(3, 3, 4)
    sums[1].finish()
    work(3, 5)
    last = sums[3]
    last.half_step(0)
    last.half_step(1)
    add(2, 4, 5)
    for stream in (*gathers, *sums[:2]):
        stream.drain()
    last.half_step(2)
    last.half_step(3)
    add(2, 6)
    last.half_step(4)
    last.half_step(5)
    sums[2].finish()
    sums[2].drain()
    last.half_step(6)
    last.finish(True)
    last.drain()


def local(features, block_values, row_ptr, block_cols):
    values, pointers, columns = block_values[0, 0], row_ptr[0, 0], block_cols[0, 0]
    side = values.shape[1]
    ranks, ring = lax.axis_size("row"), lax.axis_size("col")
    depth, width = features.shape
    lanes = 2 * width // CHUNKS
    pairs = ranks * depth // side // 2
    owned = (pointers.shape[0] - 1) * side // ring
    steps = ring - 1
    half = owned // 4
    return pl.pallas_call(
        kernel,
        out_shape=jax.ShapeDtypeStruct((owned, width), jnp.bfloat16),
        in_specs=[
            pl.BlockSpec(memory_space=pltpu.HBM),
            pl.BlockSpec(memory_space=pltpu.HBM),
            pl.BlockSpec(memory_space=pltpu.HBM),
            pl.BlockSpec(memory_space=pltpu.HBM),
            pl.BlockSpec(memory_space=pltpu.HBM),
            pl.BlockSpec(memory_space=pltpu.HBM),
        ],
        out_specs=pl.BlockSpec(memory_space=pltpu.VMEM),
        scratch_shapes=[
            pltpu.SMEM(pointers.shape, jnp.int32),
            pltpu.SMEM(columns.shape, jnp.int32),
            pltpu.VMEM((1, *pointers.shape), jnp.int32),
            pltpu.VMEM((1, *columns.shape), jnp.int32),
        ]
        + [pltpu.VMEM((pairs, side, lanes), jnp.bfloat16)] * CHUNKS
        + [
            pltpu.VMEM((depth // side, side, width), jnp.bfloat16),
            pltpu.VMEM((ROOM, side, side), jnp.bfloat16),
            pltpu.VMEM((SUMS, ROOM + 1, side, lanes), jnp.float32),
            pltpu.VMEM((ROOM, lanes), jnp.float32),
            pltpu.VMEM((ROOM, lanes), jnp.float32),
            pltpu.VMEM((owned // side // 2, side, lanes), jnp.float32),
            pltpu.VMEM((CHUNKS, 2, steps, half // side, side, lanes), jnp.int16),
            pltpu.VMEM((CHUNKS, 2, steps, half // side, side, lanes), jnp.int16),
            pltpu.VMEM((CHUNKS, 2, steps, half // side, 1, lanes), jnp.float32),
            pltpu.VMEM((CHUNKS, 2, steps, half // side, 1, lanes), jnp.float32),
            pltpu.SemaphoreType.DMA((6,)),
            pltpu.SemaphoreType.DMA((CHUNKS,)),
            pltpu.SemaphoreType.DMA((CHUNKS, EVENTS)),
            pltpu.SemaphoreType.DMA((CHUNKS,)),
            pltpu.SemaphoreType.DMA((CHUNKS,)),
            pltpu.SemaphoreType.DMA((CHUNKS + 1, steps)),
            pltpu.SemaphoreType.DMA((CHUNKS,)),
            pltpu.SemaphoreType.DMA((CHUNKS + 1, steps)),
        ],
        compiler_params=pltpu.CompilerParams(
            collective_id=0, has_side_effects=True, vmem_limit_bytes=58 * 1024 * 1024
        ),
        name="block_sparse",
    )(pointers, columns, pointers[None, :], columns[None, :], features.reshape(depth // side, side, width), values)


def solution(mesh):
    return jax.shard_map(
        local,
        mesh=mesh,
        in_specs=(
            P(("col", "row"), None),
            P("row", "col", None, None, None),
            P("row", "col", None),
            P("row", "col", None),
        ),
        out_specs=P(("row", "col"), None),
        check_vma=False,
    )
```

```python
import jax
import jax.numpy as jnp
from jax import lax
from jax.experimental import pallas as pl
from jax.experimental.pallas import tpu as pltpu
from jax.sharding import PartitionSpec as P

MESH = pl.DeviceIdType.MESH
SIDE = 4
GROUP = 8
ROOM = 144
LIMIT = 32767.0
CHUNKS = 4
EVENTS = 10
PARTS = 6
SUMS = 2


class Gather:
    def __init__(self, c, panels, send_sem, recv_sem, near_recv):
        me, self.col = lax.axis_index("row"), lax.axis_index("col")
        self.c, self.panel = c, panels[c]
        self.core, self.x, self.y = lax.rem(me, 2), lax.rem(me // 2, SIDE), me // (2 * SIDE)
        self.depth = self.panel.shape[0] // lax.axis_size("row")
        self.send_sem, self.recv_sem, self.near_recv = send_sem.at[c], recv_sem, near_recv.at[c]
        self.sent, self.due, self.near = 0, [0] * EVENTS, 0

    def rank(self, h, i, j, other=False):
        dx, dy = (i, j) if h == 0 else (j, i)
        core = 1 - self.core if other else self.core
        return (lax.rem(self.y + dy + SIDE, SIDE) * SIDE + lax.rem(self.x + dx + SIDE, SIDE)) * 2 + core

    def piece(self, h, i, j, part, other=False):
        half, quarter = self.depth // 2, self.depth // 4
        first, size = {"all": (0, half), "first": (0, quarter), "second": (quarter, quarter)}[part]
        return self.panel.at[pl.ds(self.rank(h, i, j, other) * self.depth + h * half + first, size)]

    def event(self, i, j):
        i, j = (i + 1) % SIDE - 1, (j + 1) % SIDE - 1
        return {0: 0 if i != 2 else 1, 2: 6 + i + 1}.get(j, 2 + i + 1)

    def start(self, ref, recv_sem, device):
        pltpu.make_async_remote_copy(
            src_ref=ref,
            dst_ref=ref,
            send_sem=self.send_sem,
            recv_sem=recv_sem,
            device_id=(device, self.col),
            device_id_type=MESH,
        ).start()
        self.sent += ref.shape[0]
        return ref.shape[0]

    def blocks(self, count, recv_sem):
        ref = self.panel.at[pl.ds(0, count)]
        return pltpu.make_async_remote_copy(
            src_ref=ref,
            dst_ref=ref,
            send_sem=self.send_sem,
            recv_sem=recv_sem,
            device_id=(self.rank(0, 0, 0, True), self.col),
            device_id_type=MESH,
        )

    def send(self, h, i, j, part, di, dj):
        event = self.event(i - di, j - dj)
        self.due[event] += self.start(self.piece(h, i, j, part), self.recv_sem.at[self.c, event], self.rank(h, di, dj))

    def arrive(self, i, j):
        event = self.event(i, j)
        self.blocks(self.due[event], self.recv_sem.at[self.c, event]).wait_recv()

    def hand_on(self, h, i, j):
        self.near += self.start(self.piece(h, i, j, "all"), self.near_recv, self.rank(0, 0, 0, True))

    def own(self):
        for di, dj in ((1, 0), (-1, 0), (0, 1), (0, -1)):
            for h in (0, 1):
                self.send(h, 0, 0, "all", di, dj)
        mine = self.panel.at[pl.ds(self.rank(0, 0, 0) * self.depth, self.depth)]
        self.near += self.start(mine, self.near_recv, self.rank(0, 0, 0, True))

    def forward(self, h, i, j):
        self.send(h, i, j, "first" if j == -1 else "second", 0, -j)

    def first_hop(self):
        pieces = [(h, s) for s in (-1, 1) for h in (0, 1)]
        self.arrive(1, 0)
        for h, s in pieces:
            self.send(h, s, 0, "first" if s == -1 else "second", -s, 0)
        for h, s in pieces:
            self.send(h, s, 0, "all", 0, 1)
            self.send(h, s, 0, "all", 0, -1)
        for h, s in pieces:
            self.hand_on(h, s, 0)

    def second_hop(self):
        self.arrive(2, 0)
        for h in (0, 1):
            self.send(h, 2, 0, "all", 0, 1)
            self.send(h, 2, 0, "all", 0, -1)
            self.hand_on(h, 2, 0)

    def turn(self, i, direct=False):
        self.arrive(i, 1)
        for s in (-1, 1):
            for h in (0, 1):
                self.forward(h, i, s)
                if direct:
                    part = self.piece(h, i, s, "first" if s == -1 else "second")
                    self.near += self.start(part, self.near_recv, self.rank(h, 0, -s, True))
        for s in (-1, 1):
            for h in (0, 1):
                self.hand_on(h, i, s)

    def last(self, i, direct=False):
        self.arrive(i, 2)
        if not direct:
            for h in (0, 1):
                self.hand_on(h, i, 2)

    def tail(self, direct=False):
        for i in (0, -1, 1, 2):
            self.last(i, direct and i == 2)

    def all_here(self):
        self.blocks(self.near, self.near_recv).wait_recv()

    def drain(self):
        self.blocks(self.sent, self.near_recv).wait_send()


class Reduce:
    def __init__(self, c, ptr, run, o_ref, held, sent, got, sent_scale, got_scale, sems):
        self.row, self.me, self.ring = lax.axis_index("row"), lax.axis_index("col"), lax.axis_size("col")
        self.c, self.ptr, self.run, self.o_ref, self.held = c, ptr, run, o_ref, held
        self.sent, self.got, self.sent_scale, self.got_scale, self.sems = sent, got, sent_scale, got_scale, sems
        self.side, self.lanes = run.shape[2:]
        self.pairs = o_ref.shape[0] // self.side // 2
        self.kept = {}
        self.low = lax.broadcasted_iota(jnp.int32, (self.side, self.lanes), 1) < self.lanes // 2

    def at(self, offset):
        return lax.rem(self.me + offset + self.ring, self.ring)

    def copies(self, w, *refs_and_sems):
        for a, b, s, r in refs_and_sems:
            yield pltpu.make_async_remote_copy(
                src_ref=a,
                dst_ref=b,
                send_sem=s,
                recv_sem=r,
                device_id=(self.row, self.at(1 - 2 * w)),
                device_id_type=MESH,
            )

    def both(self, at, k, j=0):
        send_sem, recv_sem, scale_send, scale_recv = self.sems
        at = (self.c, *at)
        r = self.c + j
        return (
            (self.sent.at[at], self.got.at[at], send_sem.at[self.c], recv_sem.at[r, k]),
            (self.sent_scale.at[at], self.got_scale.at[at], scale_send.at[self.c], scale_recv.at[r, k]),
        )

    def arrive(self, k, j=None):
        at = (0, pl.ds(0, 2)) if j is None else (0, 0)
        for copy in self.copies(0, *self.both(at, k, j or 0)):
            copy.wait_recv()

    def total(self, i):
        end = self.ptr[i + 1]
        return self.run[self.c % SUMS, jnp.where(end > self.ptr[i], end, 0)]

    def keep(self, stash, *places):
        for offset, h in ((0, 0), (0, 1), *places):
            for j in range(self.pairs // 2):
                n = len(self.kept)
                stash[n] = self.partial(offset, h, j)
                self.kept[(offset, h, j)] = stash.at[n]

    def partial(self, offset, h, j):
        if (offset, h, j) in self.kept:
            return self.kept[(offset, h, j)][...]
        i = (self.at(offset) * self.pairs + h * (self.pairs // 2) + j) * 2
        one, two = self.total(i), self.total(i + 1)
        return jnp.where(self.low, one, two) + self.swap(jnp.where(self.low, two, one))

    def swap(self, value):
        return pltpu.roll(value, self.lanes // 2, 1)

    def spread(self, w, k, j):
        return self.got[self.c, w, k, j].astype(jnp.int32).astype(jnp.float32) * self.got_scale[self.c, w, k, j]

    def encode(self, k, j):
        for w in (0, 1):
            offset, h = (1 - 2 * w) * (self.ring // 2 - (k + 1) // 2), w if k % 2 == 0 else 1 - w
            value = self.partial(offset, h, j)
            if k >= 2:
                value = value + self.spread(w, k - 2, j)
            top = jnp.maximum(jnp.max(jnp.abs(value), axis=0, keepdims=True), 1e-30)
            self.sent_scale[self.c, w, k, j] = top * (1.0 / LIMIT)
            self.sent[self.c, w, k, j] = jnp.round(value * (LIMIT / top)).astype(jnp.int32).astype(jnp.int16)

    def start(self, k, j=None):
        for w in (0, 1):
            for copy in self.copies(w, *self.both((w, k) if j is None else (w, k, j), k, j or 0)):
                copy.start()

    def step(self, k):
        if k >= 2:
            self.arrive(k - 2)
        for j in range(self.pairs // 2):
            self.encode(k, j)
        self.start(k)

    def half_step(self, k):
        for j in range(self.pairs // 2):
            if k >= 2:
                self.arrive(k - 2, j)
            self.encode(k, j)
            self.start(k, j)

    def finish(self, halves=False):
        last = self.ring - 2
        if not halves:
            self.arrive(last - 1)
            self.arrive(last)
        for j in range(self.pairs // 2):
            if halves:
                self.arrive(last - 1, j)
                self.arrive(last, j)
            for h in (0, 1):
                value = self.partial(0, h, j) + (self.spread(h, last, j) + self.spread(1 - h, last - 1, j))
                n = h * (self.pairs // 2) + j
                if self.c % 2 == 0:
                    self.held[n] = value
                else:
                    before = self.held[n]
                    both = jnp.where(self.low, before, self.swap(value)), jnp.where(self.low, self.swap(before), value)
                    for u in (0, 1):
                        span = pl.ds((2 * n + u) * self.side, self.side)
                        self.o_ref[span, pl.ds(self.c // 2 * self.lanes, self.lanes)] = both[u].astype(self.o_ref.dtype)

    def drain(self):
        for copy in self.copies(0, *self.both((), 0)):
            copy.wait_send()


def kernel(
    ptr_ref, cols_ref, ptr_row_ref, cols_row_ref, x_ref, a_ref, o_ref,
    ptr, cols, ptr_row, cols_row, panel_0, panel_1, panel_2, panel_3, own, values, run, same, mine, held, early, late, sent, got, sent_scale, got_scale,
    load_sem, link_send, link_recv, near_recv, send_sem, recv_sem, scale_send, scale_recv,
):
    row, col = lax.axis_index("row"), lax.axis_index("col")
    panels = (panel_0, panel_1, panel_2, panel_3)
    pairs, side, lanes = panel_0.shape
    depth = pairs // lax.axis_size("row")

    load = pltpu.make_async_copy(x_ref, own, load_sem.at[0])
    load_values = pltpu.make_async_copy(a_ref.at[pl.ds(0, ROOM)], values, load_sem.at[1])
    small = [
        pltpu.make_async_copy(a, b, load_sem.at[2 + n])
        for n, (a, b) in enumerate(((ptr_ref, ptr), (cols_ref, cols), (ptr_row_ref, ptr_row), (cols_row_ref, cols_row)))
    ]
    for copy in (load, *small, load_values):
        copy.start()

    gathers = [Gather(c, panels, link_send, link_recv, near_recv) for c in range(CHUNKS)]
    sems = (send_sem, recv_sem, scale_send, scale_recv)
    sums = [Reduce(c, ptr, run, o_ref, held, sent, got, sent_scale, got_scale, sems) for c in range(CHUNKS)]
    g, r = gathers[0], sums[0]
    barrier = pltpu.get_barrier_semaphore()
    neighbours = [(g.rank(0, i, j), col) for i, j in ((1, 0), (-1, 0), (0, 1), (0, -1))]
    neighbours += [(g.rank(0, i, j, True), col) for i, j in ((0, 0), (1, 0), (-1, 0), (0, 1), (0, -1))]
    neighbours += [(row, r.at(1)), (row, r.at(-1))]
    for device in neighbours:
        pl.semaphore_signal(barrier, inc=1, device_id=device, device_id_type=MESH)

    def pack(c):
        for n in range(depth):
            cut = pl.ds(c // 2 * lanes, lanes)
            one, two = (own[2 * n + u, :, cut].astype(jnp.float32) for u in (0, 1))
            if c % 2 == 0:
                two = r.swap(two)
            else:
                one = r.swap(one)
            panels[c][row * depth + n] = jnp.where(r.low, one, two).astype(jnp.bfloat16)

    load.wait()
    pack(0)
    pl.semaphore_wait(barrier, len(neighbours))
    gathers[0].own()
    for c in range(1, CHUNKS):
        pack(c)
    for copy in small:
        copy.wait()
    shape = (ROOM, ptr_row.shape[1])
    starts = jnp.max((lax.broadcasted_iota(jnp.int32, shape, 0) == ptr_row[...]).astype(jnp.float32), axis=1, keepdims=True)
    same[...] = jnp.broadcast_to(1.0 - starts, same.shape)
    shape = (ROOM, cols_row.shape[1])
    slot = lax.broadcasted_iota(jnp.int32, shape, 0) == lax.broadcasted_iota(jnp.int32, shape, 1)
    odd = jnp.max(jnp.where(slot, lax.rem(cols_row[...], 2), 0).astype(jnp.float32), axis=1, keepdims=True)
    high = (lax.broadcasted_iota(jnp.int32, mine.shape, 1) >= lanes // 2).astype(jnp.float32)
    mine[...] = high * odd + (1.0 - high) * (1.0 - odd)
    for n in range(SUMS):
        run[n, 0] = jnp.zeros((side, lanes), jnp.float32)

    def multiply(c, first, last):
        def step(n, carry):
            total = run[c % SUMS, n * GROUP]
            for u in range(GROUP):
                s = n * GROUP + u
                pair = lax.div(lax.rem(cols[s], 2 * pairs), 2)
                product = jnp.dot(values[s], panels[c][pair], preferred_element_type=jnp.float32)
                total = total * same[pl.ds(s, 1), :] + product * mine[pl.ds(s, 1), :]
                run[c % SUMS, s + 1] = total
            return carry

        lax.fori_loop(first, last, step, 0)

    share = ROOM // GROUP // PARTS

    def work(c, *parts):
        for part in parts:
            multiply(c, part * share, (part + 1) * share)

    def take(n, *names):
        for name in names:
            if isinstance(name, int):
                gathers[n].turn(name)
            else:
                getattr(gathers[n], name)()

    def add(n, *steps):
        for k in steps:
            sums[n].step(k)

    load_values.wait()
    take(0, "first_hop", 0, "second_hop")
    take(1, "own")
    take(0, -1, 1, 2)
    take(1, "first_hop", 0)
    take(0, "tail")
    take(1, "second_hop")
    take(2, "own")
    take(0, "all_here")
    work(0, 0, 1)
    take(1, -1)
    work(0, 2)
    take(1, 1)
    work(0, 3, 4)
    take(1, 2)
    work(0, 5)
    add(0, 0, 1)
    take(2, "first_hop", 0)
    take(1, "tail")
    take(2, "second_hop")
    take(3, "own")
    add(0, 2)
    take(1, "all_here")
    work(1, 0)
    take(2, -1)
    add(0, 3)
    work(1, 1)
    take(2, 1)
    work(1, 2, 3)
    take(2, 2)
    work(1, 4)
    add(0, 4)
    work(1, 5)
    take(3, "first_hop")
    add(1, 0, 1)
    add(0, 5)
    take(3, 0)
    take(2, "tail")
    take(3, "second_hop")
    add(0, 6)
    sums[0].keep(early)
    take(2, "all_here")
    take(3, -1)
    work(2, 0)
    add(1, 2)
    work(2, 1)
    take(3, 1)
    add(1, 3)
    work(2, 2, 3)
    gathers[3].turn(2, True)
    work(2, 4, 5)
    add(2, 0, 1)
    sums[0].finish()
    add(1, 4, 5)
    sums[1].keep(late, (1, 0), (-1, 1))
    gathers[3].tail(True)
    take(3, "all_here")
    work(3, 0, 1)
    add(2, 2)
    work(3, 2)
    add(1, 6)
    add(2, 3)
    work(3, 3, 4, 5)
    last = sums[3]
    last.half_step(0)
    last.half_step(1)
    add(2, 4)
    sums[1].finish()
    for stream in (*gathers, *sums[:2]):
        stream.drain()
    last.half_step(2)
    last.half_step(3)
    add(2, 5)
    last.half_step(4)
    add(2, 6)
    last.half_step(5)
    last.half_step(6)
    sums[2].finish()
    sums[2].drain()
    last.finish(True)
    last.drain()


def local(features, block_values, row_ptr, block_cols):
    values, pointers, columns = block_values[0, 0], row_ptr[0, 0], block_cols[0, 0]
    side = values.shape[1]
    ranks, ring = lax.axis_size("row"), lax.axis_size("col")
    depth, width = features.shape
    lanes = 2 * width // CHUNKS
    pairs = ranks * depth // side // 2
    owned = (pointers.shape[0] - 1) * side // ring
    steps = ring - 1
    half = owned // 4
    return pl.pallas_call(
        kernel,
        out_shape=jax.ShapeDtypeStruct((owned, width), jnp.bfloat16),
        in_specs=[
            pl.BlockSpec(memory_space=pltpu.HBM),
            pl.BlockSpec(memory_space=pltpu.HBM),
            pl.BlockSpec(memory_space=pltpu.HBM),
            pl.BlockSpec(memory_space=pltpu.HBM),
            pl.BlockSpec(memory_space=pltpu.HBM),
            pl.BlockSpec(memory_space=pltpu.HBM),
        ],
        out_specs=pl.BlockSpec(memory_space=pltpu.VMEM),
        scratch_shapes=[
            pltpu.SMEM(pointers.shape, jnp.int32),
            pltpu.SMEM(columns.shape, jnp.int32),
            pltpu.VMEM((1, *pointers.shape), jnp.int32),
            pltpu.VMEM((1, *columns.shape), jnp.int32),
        ]
        + [pltpu.VMEM((pairs, side, lanes), jnp.bfloat16)] * CHUNKS
        + [
            pltpu.VMEM((depth // side, side, width), jnp.bfloat16),
            pltpu.VMEM((ROOM, side, side), jnp.bfloat16),
            pltpu.VMEM((SUMS, ROOM + 1, side, lanes), jnp.float32),
            pltpu.VMEM((ROOM, lanes), jnp.float32),
            pltpu.VMEM((ROOM, lanes), jnp.float32),
            pltpu.VMEM((owned // side // 2, side, lanes), jnp.float32),
            pltpu.VMEM((owned // side // 2, side, lanes), jnp.float32),
            pltpu.VMEM((owned // side, side, lanes), jnp.float32),
            pltpu.VMEM((CHUNKS, 2, steps, half // side, side, lanes), jnp.int16),
            pltpu.VMEM((CHUNKS, 2, steps, half // side, side, lanes), jnp.int16),
            pltpu.VMEM((CHUNKS, 2, steps, half // side, 1, lanes), jnp.float32),
            pltpu.VMEM((CHUNKS, 2, steps, half // side, 1, lanes), jnp.float32),
            pltpu.SemaphoreType.DMA((6,)),
            pltpu.SemaphoreType.DMA((CHUNKS,)),
            pltpu.SemaphoreType.DMA((CHUNKS, EVENTS)),
            pltpu.SemaphoreType.DMA((CHUNKS,)),
            pltpu.SemaphoreType.DMA((CHUNKS,)),
            pltpu.SemaphoreType.DMA((CHUNKS + 1, steps)),
            pltpu.SemaphoreType.DMA((CHUNKS,)),
            pltpu.SemaphoreType.DMA((CHUNKS + 1, steps)),
        ],
        compiler_params=pltpu.CompilerParams(
            collective_id=0, has_side_effects=True, vmem_limit_bytes=50 * 1024 * 1024
        ),
        name="block_sparse",
    )(
        *(
            pltpu.with_memory_space_constraint(operand, pltpu.HBM)
            for operand in (
                pointers,
                columns,
                pointers[None, :],
                columns[None, :],
                features.reshape(depth // side, side, width),
                values,
            )
        )
    )


def solution(mesh):
    return jax.shard_map(
        local,
        mesh=mesh,
        in_specs=(
            P(("col", "row"), None),
            P("row", "col", None, None, None),
            P("row", "col", None),
            P("row", "col", None),
        ),
        out_specs=P(("row", "col"), None),
        check_vma=False,
    )
```

```python
import jax
import jax.numpy as jnp
from jax import lax
from jax.experimental import pallas as pl
from jax.experimental.pallas import tpu as pltpu
from jax.sharding import PartitionSpec as P

MESH = pl.DeviceIdType.MESH
SIDE = 4
GROUP = 8
ROOM = 144
LIMIT = 32767.0
CHUNKS = 4
EVENTS = 10
PARTS = 6
SUMS = 2


class Gather:
    def __init__(self, c, panels, send_sem, recv_sem, near_recv):
        me, self.col = lax.axis_index("row"), lax.axis_index("col")
        self.c, self.panel = c, panels[c]
        self.core, self.x, self.y = lax.rem(me, 2), lax.rem(me // 2, SIDE), me // (2 * SIDE)
        self.depth = self.panel.shape[0] // lax.axis_size("row")
        self.send_sem, self.recv_sem, self.near_recv = send_sem.at[c], recv_sem, near_recv.at[c]
        self.sent, self.due, self.near = 0, [0] * EVENTS, 0

    def rank(self, h, i, j, other=False):
        dx, dy = (i, j) if h == 0 else (j, i)
        core = 1 - self.core if other else self.core
        return (lax.rem(self.y + dy + SIDE, SIDE) * SIDE + lax.rem(self.x + dx + SIDE, SIDE)) * 2 + core

    def piece(self, h, i, j, part, other=False):
        half, quarter = self.depth // 2, self.depth // 4
        first, size = {"all": (0, half), "first": (0, quarter), "second": (quarter, quarter)}[part]
        return self.panel.at[pl.ds(self.rank(h, i, j, other) * self.depth + h * half + first, size)]

    def event(self, i, j):
        i, j = (i + 1) % SIDE - 1, (j + 1) % SIDE - 1
        return {0: 0 if i != 2 else 1, 2: 6 + i + 1}.get(j, 2 + i + 1)

    def start(self, ref, recv_sem, device):
        pltpu.make_async_remote_copy(
            src_ref=ref,
            dst_ref=ref,
            send_sem=self.send_sem,
            recv_sem=recv_sem,
            device_id=(device, self.col),
            device_id_type=MESH,
        ).start()
        self.sent += ref.shape[0]
        return ref.shape[0]

    def blocks(self, count, recv_sem):
        ref = self.panel.at[pl.ds(0, count)]
        return pltpu.make_async_remote_copy(
            src_ref=ref,
            dst_ref=ref,
            send_sem=self.send_sem,
            recv_sem=recv_sem,
            device_id=(self.rank(0, 0, 0, True), self.col),
            device_id_type=MESH,
        )

    def send(self, h, i, j, part, di, dj):
        event = self.event(i - di, j - dj)
        self.due[event] += self.start(self.piece(h, i, j, part), self.recv_sem.at[self.c, event], self.rank(h, di, dj))

    def arrive(self, i, j):
        event = self.event(i, j)
        self.blocks(self.due[event], self.recv_sem.at[self.c, event]).wait_recv()

    def hand_on(self, h, i, j):
        self.near += self.start(self.piece(h, i, j, "all"), self.near_recv, self.rank(0, 0, 0, True))

    def own(self):
        for di, dj in ((1, 0), (-1, 0), (0, 1), (0, -1)):
            for h in (0, 1):
                self.send(h, 0, 0, "all", di, dj)
        mine = self.panel.at[pl.ds(self.rank(0, 0, 0) * self.depth, self.depth)]
        self.near += self.start(mine, self.near_recv, self.rank(0, 0, 0, True))

    def forward(self, h, i, j):
        self.send(h, i, j, "first" if j == -1 else "second", 0, -j)

    def first_hop(self):
        pieces = [(h, s) for s in (-1, 1) for h in (0, 1)]
        self.arrive(1, 0)
        for h, s in pieces:
            self.send(h, s, 0, "first" if s == -1 else "second", -s, 0)
        for h, s in pieces:
            self.send(h, s, 0, "all", 0, 1)
            self.send(h, s, 0, "all", 0, -1)
        for h, s in pieces:
            self.hand_on(h, s, 0)

    def second_hop(self):
        self.arrive(2, 0)
        for h in (0, 1):
            self.send(h, 2, 0, "all", 0, 1)
            self.send(h, 2, 0, "all", 0, -1)
            self.hand_on(h, 2, 0)

    def turn(self, i, direct=False):
        self.arrive(i, 1)
        for s in (-1, 1):
            for h in (0, 1):
                self.forward(h, i, s)
                if direct:
                    part = self.piece(h, i, s, "first" if s == -1 else "second")
                    self.near += self.start(part, self.near_recv, self.rank(h, 0, -s, True))
        for s in (-1, 1):
            for h in (0, 1):
                self.hand_on(h, i, s)

    def last(self, i, direct=False):
        self.arrive(i, 2)
        if not direct:
            for h in (0, 1):
                self.hand_on(h, i, 2)

    def tail(self, direct=False):
        for i in (0, -1, 1, 2):
            self.last(i, direct and i == 2)

    def all_here(self):
        self.blocks(self.near, self.near_recv).wait_recv()

    def drain(self):
        self.blocks(self.sent, self.near_recv).wait_send()


class Reduce:
    def __init__(self, c, ptr, run, o_ref, held, sent, got, sent_scale, got_scale, sems):
        self.row, self.me, self.ring = lax.axis_index("row"), lax.axis_index("col"), lax.axis_size("col")
        self.c, self.ptr, self.run, self.o_ref, self.held = c, ptr, run, o_ref, held
        self.sent, self.got, self.sent_scale, self.got_scale, self.sems = sent, got, sent_scale, got_scale, sems
        self.side, self.lanes = run.shape[2:]
        self.pairs = o_ref.shape[0] // self.side // 2
        self.kept = {}
        self.low = lax.broadcasted_iota(jnp.int32, (self.side, self.lanes), 1) < self.lanes // 2

    def at(self, offset):
        return lax.rem(self.me + offset + self.ring, self.ring)

    def copies(self, w, *refs_and_sems):
        for a, b, s, r in refs_and_sems:
            yield pltpu.make_async_remote_copy(
                src_ref=a,
                dst_ref=b,
                send_sem=s,
                recv_sem=r,
                device_id=(self.row, self.at(1 - 2 * w)),
                device_id_type=MESH,
            )

    def both(self, at, k, j=0):
        send_sem, recv_sem, scale_send, scale_recv = self.sems
        at = (self.c, *at)
        r = self.c + j
        return (
            (self.sent.at[at], self.got.at[at], send_sem.at[self.c], recv_sem.at[r, k]),
            (self.sent_scale.at[at], self.got_scale.at[at], scale_send.at[self.c], scale_recv.at[r, k]),
        )

    def arrive(self, k, j=None):
        at = (0, pl.ds(0, 2)) if j is None else (0, 0)
        for copy in self.copies(0, *self.both(at, k, j or 0)):
            copy.wait_recv()

    def total(self, i):
        end = self.ptr[i + 1]
        return self.run[self.c % SUMS, jnp.where(end > self.ptr[i], end, 0)]

    def keep(self, stash, *places):
        for offset, h in ((0, 0), (0, 1), *places):
            for j in range(self.pairs // 2):
                n = len(self.kept)
                stash[n] = self.partial(offset, h, j)
                self.kept[(offset, h, j)] = stash.at[n]

    def partial(self, offset, h, j):
        if (offset, h, j) in self.kept:
            return self.kept[(offset, h, j)][...]
        i = (self.at(offset) * self.pairs + h * (self.pairs // 2) + j) * 2
        one, two = self.total(i), self.total(i + 1)
        return jnp.where(self.low, one, two) + self.swap(jnp.where(self.low, two, one))

    def swap(self, value):
        return pltpu.roll(value, self.lanes // 2, 1)

    def spread(self, w, k, j):
        return self.got[self.c, w, k, j].astype(jnp.int32).astype(jnp.float32) * self.got_scale[self.c, w, k, j]

    def encode(self, k, j):
        for w in (0, 1):
            offset, h = (1 - 2 * w) * (self.ring // 2 - (k + 1) // 2), w if k % 2 == 0 else 1 - w
            value = self.partial(offset, h, j)
            if k >= 2:
                value = value + self.spread(w, k - 2, j)
            top = jnp.maximum(jnp.max(jnp.abs(value), axis=0, keepdims=True), 1e-30)
            self.sent_scale[self.c, w, k, j] = top * (1.0 / LIMIT)
            self.sent[self.c, w, k, j] = jnp.round(value * (LIMIT / top)).astype(jnp.int32).astype(jnp.int16)

    def start(self, k, j=None):
        for w in (0, 1):
            for copy in self.copies(w, *self.both((w, k) if j is None else (w, k, j), k, j or 0)):
                copy.start()

    def step(self, k):
        if k >= 2:
            self.arrive(k - 2)
        for j in range(self.pairs // 2):
            self.encode(k, j)
        self.start(k)

    def half_step(self, k):
        for j in range(self.pairs // 2):
            if k >= 2:
                self.arrive(k - 2, j)
            self.encode(k, j)
            self.start(k, j)

    def finish(self, halves=False):
        last = self.ring - 2
        if not halves:
            self.arrive(last - 1)
            self.arrive(last)
        for j in range(self.pairs // 2):
            if halves:
                self.arrive(last - 1, j)
                self.arrive(last, j)
            for h in (0, 1):
                value = self.partial(0, h, j) + (self.spread(h, last, j) + self.spread(1 - h, last - 1, j))
                n = h * (self.pairs // 2) + j
                if self.c % 2 == 0:
                    self.held[n] = value
                else:
                    before = self.held[n]
                    both = jnp.where(self.low, before, self.swap(value)), jnp.where(self.low, self.swap(before), value)
                    for u in (0, 1):
                        span = pl.ds((2 * n + u) * self.side, self.side)
                        self.o_ref[span, pl.ds(self.c // 2 * self.lanes, self.lanes)] = both[u].astype(self.o_ref.dtype)

    def drain(self):
        for copy in self.copies(0, *self.both((), 0)):
            copy.wait_send()


def kernel(
    ptr_ref, cols_ref, ptr_row_ref, cols_row_ref, x_ref, a_ref, o_ref,
    ptr, cols, ptr_row, cols_row, panel_0, panel_1, panel_2, panel_3, own, values, run, same, mine, held, early, late, sent, got, sent_scale, got_scale,
    load_sem, link_send, link_recv, near_recv, send_sem, recv_sem, scale_send, scale_recv,
):
    row, col = lax.axis_index("row"), lax.axis_index("col")
    panels = (panel_0, panel_1, panel_2, panel_3)
    pairs, side, lanes = panel_0.shape
    depth = pairs // lax.axis_size("row")

    load = pltpu.make_async_copy(x_ref, own, load_sem.at[0])
    load_values = pltpu.make_async_copy(a_ref.at[pl.ds(0, ROOM)], values, load_sem.at[1])
    small = [
        pltpu.make_async_copy(a, b, load_sem.at[2 + n])
        for n, (a, b) in enumerate(((ptr_ref, ptr), (cols_ref, cols), (ptr_row_ref, ptr_row), (cols_row_ref, cols_row)))
    ]
    for copy in (load, *small, load_values):
        copy.start()

    gathers = [Gather(c, panels, link_send, link_recv, near_recv) for c in range(CHUNKS)]
    sems = (send_sem, recv_sem, scale_send, scale_recv)
    sums = [Reduce(c, ptr, run, o_ref, held, sent, got, sent_scale, got_scale, sems) for c in range(CHUNKS)]
    g, r = gathers[0], sums[0]
    barrier = pltpu.get_barrier_semaphore()
    neighbours = [(g.rank(0, i, j), col) for i, j in ((1, 0), (-1, 0), (0, 1), (0, -1))]
    neighbours += [(g.rank(0, i, j, True), col) for i, j in ((0, 0), (1, 0), (-1, 0), (0, 1), (0, -1))]
    neighbours += [(row, r.at(1)), (row, r.at(-1))]
    for device in neighbours:
        pl.semaphore_signal(barrier, inc=1, device_id=device, device_id_type=MESH)

    def pack(c):
        for n in range(depth):
            cut = pl.ds(c // 2 * lanes, lanes)
            one, two = (own[2 * n + u, :, cut].astype(jnp.float32) for u in (0, 1))
            if c % 2 == 0:
                two = r.swap(two)
            else:
                one = r.swap(one)
            panels[c][row * depth + n] = jnp.where(r.low, one, two).astype(jnp.bfloat16)

    load.wait()
    pack(0)
    pl.semaphore_wait(barrier, len(neighbours))
    gathers[0].own()
    for c in range(1, CHUNKS):
        pack(c)
    for copy in small:
        copy.wait()
    shape = (ROOM, ptr_row.shape[1])
    starts = jnp.max((lax.broadcasted_iota(jnp.int32, shape, 0) == ptr_row[...]).astype(jnp.float32), axis=1, keepdims=True)
    same[...] = jnp.broadcast_to(1.0 - starts, same.shape)
    shape = (ROOM, cols_row.shape[1])
    slot = lax.broadcasted_iota(jnp.int32, shape, 0) == lax.broadcasted_iota(jnp.int32, shape, 1)
    odd = jnp.max(jnp.where(slot, lax.rem(cols_row[...], 2), 0).astype(jnp.float32), axis=1, keepdims=True)
    high = (lax.broadcasted_iota(jnp.int32, mine.shape, 1) >= lanes // 2).astype(jnp.float32)
    mine[...] = high * odd + (1.0 - high) * (1.0 - odd)
    for n in range(SUMS):
        run[n, 0] = jnp.zeros((side, lanes), jnp.float32)

    def multiply(c, first, last):
        def step(n, carry):
            total = run[c % SUMS, n * GROUP]
            for u in range(GROUP):
                s = n * GROUP + u
                pair = lax.div(lax.rem(cols[s], 2 * pairs), 2)
                product = jnp.dot(values[s], panels[c][pair], preferred_element_type=jnp.float32)
                total = total * same[pl.ds(s, 1), :] + product * mine[pl.ds(s, 1), :]
                run[c % SUMS, s + 1] = total
            return carry

        lax.fori_loop(first, last, step, 0)

    share = ROOM // GROUP // PARTS

    def work(c, *parts):
        for part in parts:
            multiply(c, part * share, (part + 1) * share)

    def take(n, *names):
        for name in names:
            if isinstance(name, int):
                gathers[n].turn(name)
            else:
                getattr(gathers[n], name)()

    def add(n, *steps):
        for k in steps:
            sums[n].step(k)

    load_values.wait()
    take(0, "first_hop", 0, "second_hop")
    take(1, "own")
    take(0, -1, 1, 2)
    take(1, "first_hop", 0)
    take(0, "tail")
    take(1, "second_hop")
    take(2, "own")
    take(0, "all_here")
    work(0, 0, 1)
    take(1, -1)
    work(0, 2)
    take(1, 1)
    work(0, 3, 4)
    take(1, 2)
    work(0, 5)
    add(0, 0, 1)
    take(2, "first_hop", 0)
    take(1, "tail")
    take(2, "second_hop")
    take(3, "own")
    add(0, 2)
    take(1, "all_here")
    work(1, 0)
    take(2, -1)
    add(0, 3)
    work(1, 1)
    take(2, 1)
    work(1, 2, 3)
    take(2, 2)
    work(1, 4)
    add(0, 4)
    work(1, 5)
    take(3, "first_hop")
    add(1, 0, 1)
    add(0, 5)
    take(3, 0)
    take(2, "tail")
    take(3, "second_hop")
    add(0, 6)
    sums[0].keep(early)
    take(2, "all_here")
    take(3, -1)
    work(2, 0)
    add(1, 2)
    work(2, 1)
    take(3, 1)
    add(1, 3)
    work(2, 2, 3)
    gathers[3].turn(2, True)
    work(2, 4, 5)
    add(2, 0, 1)
    sums[0].finish()
    add(1, 4, 5)
    sums[1].keep(late, (1, 0), (-1, 1))
    gathers[3].tail(True)
    take(3, "all_here")
    work(3, 0, 1, 2)
    add(2, 2)
    work(3, 3)
    add(1, 6)
    add(2, 3)
    work(3, 4, 5)
    last = sums[3]
    last.half_step(0)
    last.half_step(1)
    add(2, 4)
    for stream in (*gathers, sums[0]):
        stream.drain()
    last.half_step(2)
    sums[1].finish()
    sums[1].drain()
    last.half_step(3)
    add(2, 5)
    last.half_step(4)
    add(2, 6)
    last.half_step(5)
    last.half_step(6)
    sums[2].finish()
    sums[2].drain()
    last.finish(True)
    last.drain()


def local(features, block_values, row_ptr, block_cols):
    values, pointers, columns = block_values[0, 0], row_ptr[0, 0], block_cols[0, 0]
    side = values.shape[1]
    ranks, ring = lax.axis_size("row"), lax.axis_size("col")
    depth, width = features.shape
    lanes = 2 * width // CHUNKS
    pairs = ranks * depth // side // 2
    owned = (pointers.shape[0] - 1) * side // ring
    steps = ring - 1
    half = owned // 4
    return pl.pallas_call(
        kernel,
        out_shape=jax.ShapeDtypeStruct((owned, width), jnp.bfloat16),
        in_specs=[
            pl.BlockSpec(memory_space=pltpu.HBM),
            pl.BlockSpec(memory_space=pltpu.HBM),
            pl.BlockSpec(memory_space=pltpu.HBM),
            pl.BlockSpec(memory_space=pltpu.HBM),
            pl.BlockSpec(memory_space=pltpu.HBM),
            pl.BlockSpec(memory_space=pltpu.HBM),
        ],
        out_specs=pl.BlockSpec(memory_space=pltpu.VMEM),
        scratch_shapes=[
            pltpu.SMEM(pointers.shape, jnp.int32),
            pltpu.SMEM(columns.shape, jnp.int32),
            pltpu.VMEM((1, *pointers.shape), jnp.int32),
            pltpu.VMEM((1, *columns.shape), jnp.int32),
        ]
        + [pltpu.VMEM((pairs, side, lanes), jnp.bfloat16)] * CHUNKS
        + [
            pltpu.VMEM((depth // side, side, width), jnp.bfloat16),
            pltpu.VMEM((ROOM, side, side), jnp.bfloat16),
            pltpu.VMEM((SUMS, ROOM + 1, side, lanes), jnp.float32),
            pltpu.VMEM((ROOM, lanes), jnp.float32),
            pltpu.VMEM((ROOM, lanes), jnp.float32),
            pltpu.VMEM((owned // side // 2, side, lanes), jnp.float32),
            pltpu.VMEM((owned // side // 2, side, lanes), jnp.float32),
            pltpu.VMEM((owned // side, side, lanes), jnp.float32),
            pltpu.VMEM((CHUNKS, 2, steps, half // side, side, lanes), jnp.int16),
            pltpu.VMEM((CHUNKS, 2, steps, half // side, side, lanes), jnp.int16),
            pltpu.VMEM((CHUNKS, 2, steps, half // side, 1, lanes), jnp.float32),
            pltpu.VMEM((CHUNKS, 2, steps, half // side, 1, lanes), jnp.float32),
            pltpu.SemaphoreType.DMA((6,)),
            pltpu.SemaphoreType.DMA((CHUNKS,)),
            pltpu.SemaphoreType.DMA((CHUNKS, EVENTS)),
            pltpu.SemaphoreType.DMA((CHUNKS,)),
            pltpu.SemaphoreType.DMA((CHUNKS,)),
            pltpu.SemaphoreType.DMA((CHUNKS + 1, steps)),
            pltpu.SemaphoreType.DMA((CHUNKS,)),
            pltpu.SemaphoreType.DMA((CHUNKS + 1, steps)),
        ],
        compiler_params=pltpu.CompilerParams(
            collective_id=0, has_side_effects=True, vmem_limit_bytes=50 * 1024 * 1024
        ),
        name="block_sparse",
    )(
        *(
            pltpu.with_memory_space_constraint(operand, pltpu.HBM)
            for operand in (
                pointers,
                columns,
                pointers[None, :],
                columns[None, :],
                features.reshape(depth // side, side, width),
                values,
            )
        )
    )


def solution(mesh):
    return jax.shard_map(
        local,
        mesh=mesh,
        in_specs=(
            P(("col", "row"), None),
            P("row", "col", None, None, None),
            P("row", "col", None),
            P("row", "col", None),
        ),
        out_specs=P(("row", "col"), None),
        check_vma=False,
    )
```
